512 devices in a mesh: row: 16 (over x, z_hi), col: 8 (over y, core), layer: 4 (over z_lo).
Axes of the slice: x: 4, y: 4, z: 16 (z_hi: 4, z_lo: 4; z = z_hi * 4 + z_lo), core: 2. Of those that a mesh axis runs over, the one named last changes fastest.
Arguments:
- design: float32 [4096, 8192], P(('row', 'layer'), 'col'), may hold values from -6 to 6
- responses: float32 [4096, 8192], P(('row', 'layer'), 'col'), may hold values from -0.09375 to 0.09375
Outputs:
- normal_update: float32 [8192, 8192], P('row', ('col', 'layer'))
The draws below stay inside these ranges and needn't reach their ends.
All inputs are finite; a program needn't handle non-finite values.
Results may differ from the reference program's by a relative error of at most 0.00008.
Values sent between devices are 32-bit elements; how exact they have to be, the bound alone decides.
A program may use at most 64 MiB of HBM per device.

```python
import jax
import jax.numpy as jnp
from jax import lax

NA = 8192
NB = 8192
K = 4096


def block_levels(rng, dims, pieces, least, high):
    gain, own = 1.0, jax.random.fold_in(rng, 6)
    for axis_at, shards_of in pieces:
        heights = jnp.exp(jax.random.uniform(jax.random.fold_in(own, axis_at), (shards_of,), jnp.float32, least / len(pieces), high / len(pieces)))
        gain = gain * jnp.repeat(heights, dims[axis_at] // shards_of).reshape([-1 if axis == axis_at else 1 for axis in range(len(dims))])
    return gain


def noise(stream_key, extent, spread, bound, split=(), dtype=jnp.bfloat16):
    values = spread * jax.random.normal(stream_key, extent, jnp.float32)
    if split:
        values = values * block_levels(stream_key, extent, split, -0.22, 0.18)
    return jnp.clip(values, -bound, bound).astype(dtype)


def setup_inputs(seed: int = 0) -> dict:
    seeds = jax.random.split(jax.random.key(seed), 3)
    return {
        "design": noise(seeds[0], (K, NA), 1.0, 6.0, ((0, 64), (1, 8)), jnp.float32),
        "responses": noise(seeds[1], (K, NB), K ** -0.5, 0.09375, ((0, 64), (1, 8)), jnp.float32),
    }


def reference(design, responses):
    transposed = jnp.transpose(design)
    return jnp.dot(transposed, responses, precision=lax.Precision.HIGHEST, preferred_element_type=jnp.float32)
```

```python
import jax
import jax.numpy as jnp
from jax import lax
from jax.experimental import pallas as pl
from jax.experimental.pallas import tpu as pltpu
from jax.sharding import Mesh
from jax.sharding import PartitionSpec as P

MESH = pl.DeviceIdType.MESH
F32, BF16 = jnp.float32, jnp.bfloat16


def split(value):
    high = value.astype(BF16)
    return high, (value - high.astype(F32)).astype(BF16)


PIECES = (
    [(64 * s, 64) for s in range(8)]
    + [(512, 32)]
    + [(64 * s, 64) for s in range(9, 16)]
    + [(544, 32)]
)
DIRECT = [15, 1, 14, 2, 13, 3, 12, 4]
RELAYED = [11, 5, 10, 6, 9, 7, 16, 8]


def kernel(d_hbm, r_hbm, o_ref, dv, rv, turned, dbuf, rbuf, dth, dtl, local, ss, dz, dy, dd, tz, rz, rx):
    x, zh, y, c, p = (lax.axis_index(n) for n in ("x", "zh", "y", "c", "p"))
    z = 4 * zh + p

    def ring(v, n):
        return lax.rem(v + 4 * n, n)

    def at_z(d):
        w = ring(z + d, 16)
        return {"zh": lax.div(w, 4), "p": lax.rem(w, 4)}

    up_x, down_x = {"x": ring(x + 1, 4)}, {"x": ring(x - 1, 4)}
    up_y, down_y = {"y": ring(y + 1, 4)}, {"y": ring(y - 1, 4)}
    partner = {"c": 1 - c}

    started = []

    def send(src, dst, sem, device, when=None):
        number = len(started)
        copy = pltpu.make_async_remote_copy(
            src_ref=src,
            dst_ref=dst,
            send_sem=ss.at[number],
            recv_sem=sem,
            device_id=device,
            device_id_type=MESH,
        )
        started.append((copy, when))
        if when is None:
            copy.start()
        else:
            pl.when(when)(copy.start)

    def arrived(dst, sem, when=None):
        copy = pltpu.make_async_copy(dst, dst, sem)
        if when is None:
            copy.wait()
        else:
            pl.when(when)(copy.wait)

    load_d = pltpu.make_async_copy(d_hbm, dv, local.at[0])
    load_r = pltpu.make_async_copy(r_hbm, rv, local.at[1])
    own = r_hbm.at[:, pl.ds(pl.multiple_of(p * 256, 256), 256)]
    load_own = pltpu.make_async_copy(own, rbuf.at[x, pl.ds(0, 64)], local.at[2])
    load_d.start()
    load_r.start()
    load_own.start()

    barrier = pltpu.get_barrier_semaphore()

    def greet(device, when=None):
        def signal():
            pl.semaphore_signal(barrier, inc=1, device_id=device, device_id_type=MESH)

        if when is None:
            signal()
        else:
            pl.when(when)(signal)

    source_core = lax.div(zh, 2)
    for d in (1, -1, 2, -2, 3, -3, 4, -4):
        greet(at_z(d))
    for device in (up_x, down_x, up_y, down_y, partner):
        greet(device)
    for other in range(4):
        greet({"x": other, "y": x}, jnp.logical_or(x != other, y != x))

    def origin(r, ps):
        return {"zh": ring(zh - r, 4), "p": ps, "c": source_core}

    def upward(r, ps):
        return r == 1 or (r == 2 and ps >= 2)

    for r in (1, 3, 2):
        for ps in range(4):
            greet(origin(r, ps), p == (0 if upward(r, ps) else 3))
    diagonal = x == y
    holder = c == source_core
    pl.semaphore_wait(
        barrier,
        4 - diagonal.astype(jnp.int32) + 8 + 5 + jnp.where(holder, 2, 4),
    )

    load_d.wait()
    for part in range(4):
        send(
            dv.at[pl.ds(16 * part, 16)],
            turned.at[x],
            tz.at[x],
            {"x": y, "y": part},
            jnp.logical_or(x != y, y != part),
        )

    @pl.when(diagonal)
    def _():
        turned[x] = dv[pl.ds(pl.multiple_of(16 * y, 16), 16), :]

    def piece(number, owner, rows=None):
        first, count = PIECES[number]
        if rows is not None:
            first, count = first + rows * (count // 2), count // 2
        return rbuf.at[owner, pl.ds(first, count)]

    def along_x(number):
        for side, device in ((0, up_x), (1, down_x)):
            send(piece(number, x), piece(number, x), rx.at[side, number], device)

    load_own.wait()
    along_x(0)
    load_r.wait()
    for d in (1, -1, 2, -2, 3, -3, 4, -4):
        quarter = pl.ds(pl.multiple_of(ring(p + d, 4) * 256, 256), 256)
        slot = (-d) % 16
        send(rv.at[:, quarter], piece(slot, x), rz.at[slot], at_z(d))

    for other in range(4):
        arrived(
            turned.at[other],
            tz.at[other],
            jnp.logical_or(x != other, y != x),
        )

    def block(core, slot):
        return dbuf.at[core, pl.ds(4 * slot, 4), y]

    for h in range(2):
        target = 2 * c + h
        rel = ring(target - zh, 4)
        up = jnp.logical_or(rel == 1, jnp.logical_and(rel == 2, p >= 2))
        entry = jnp.where(rel == 0, p, jnp.where(up, 0, 3))
        slot = 4 * rel + p
        for core in range(2):
            columns = pl.ds(512 * h + 256 * core, 256)
            mine = jnp.logical_and(rel == 0, c == core)
            send(
                turned.at[:, :, columns],
                block(core, slot),
                dz.at[slot],
                {"zh": target, "p": entry, "c": core},
                jnp.logical_not(mine),
            )

            @pl.when(mine)
            def _():
                dbuf[core, pl.ds(4 * p, 4), y] = turned[:, :, columns]

    above, below = at_z(1), at_z(-1)

    def design_slot(r, ps):
        slot = 4 * r + ps
        here = block(c, slot)
        if r == 0:
            arrived(here, dz.at[slot], jnp.logical_not(jnp.logical_and(p == ps, holder)))
            goes_up = jnp.logical_and(p >= ps, p < 3) if ps < 3 else None
            goes_down = jnp.logical_and(p <= ps, p > 0) if ps > 0 else None
        else:
            arrived(here, dz.at[slot])
            goes_up = p < 3 if upward(r, ps) else None
            goes_down = None if upward(r, ps) else p > 0
        if goes_up is not None:
            send(here, here, dz.at[slot], above, goes_up)
        if goes_down is not None:
            send(here, here, dz.at[slot], below, goes_down)

    def group(core, r, part, half=None):
        first, count = (16 * r, 16) if half is None else (16 * r + 8 * half, 8)
        return dbuf.at[core, pl.ds(first, count), part]

    y_of = [y, ring(y - 1, 4), ring(y + 1, 4), ring(y + 2, 4)]

    def to_partner(r, which):
        send(group(c, r, y_of[which]), group(c, r, y_of[which]), dd.at[r, which], partner)

    def along_y(r):
        send(group(c, r, y), group(c, r, y), dy.at[0, r], up_y)
        send(group(c, r, y), group(c, r, y), dy.at[1, r], down_y)
        to_partner(r, 0)

    def relay_y(r):
        arrived(group(c, r, y_of[1]), dy.at[0, r])
        send(group(c, r, y_of[1], 0), group(c, r, y_of[1], 0), dy.at[2, r], up_y)
        to_partner(r, 1)
        arrived(group(c, r, y_of[2]), dy.at[1, r])
        send(group(c, r, y_of[2], 1), group(c, r, y_of[2], 1), dy.at[3, r], down_y)
        to_partner(r, 2)

    def last_y(r):
        arrived(group(c, r, y_of[3], 0), dy.at[2, r])
        arrived(group(c, r, y_of[3], 1), dy.at[3, r])
        to_partner(r, 3)

    left, right, far = ring(x - 1, 4), ring(x + 1, 4), ring(x + 2, 4)

    def from_z(number):
        arrived(piece(number, x), rz.at[number])
        along_x(number)

    def relay_z(number):
        if number >= 12:
            there = 16 if number == 12 else number - 4
            half = 1 if number == 12 else None
            device = at_z(4)
        else:
            there = number + 4
            half = 0 if number == 4 else None
            device = at_z(-4)
        send(piece(number, x, half), piece(there, x), rz.at[there], device)

    def relay_x(number):
        arrived(piece(number, left), rx.at[0, number])
        send(piece(number, left, 0), piece(number, left, 0), rx.at[2, number], up_x)
        arrived(piece(number, right), rx.at[1, number])
        send(piece(number, right, 1), piece(number, right, 1), rx.at[3, number], down_x)

    def last_x(number):
        arrived(piece(number, far, 0), rx.at[2, number])
        arrived(piece(number, far, 1), rx.at[3, number])

    def prepare(r):
        for which in range(4):
            arrived(group(1 - c, r, y_of[which]), dd.at[r, which])

        @pl.loop(0, 4)
        def _(ps):
            slot = 4 * r + ps
            for half in range(2):
                value = dbuf[half, pl.ds(4 * slot, 4)].reshape(256, 256).T
                high, low = split(value)
                dth[slot, pl.ds(256 * half, 256), :] = high
                dtl[slot, pl.ds(256 * half, 256), :] = low

    def multiply(slot):
        owner = ring(z + slot, 16)
        other = 4 * ring(zh - lax.div(owner, 4), 4) + lax.rem(owner, 4)
        rows = pl.ds(pl.multiple_of(64 * slot, 64), 64)
        high, low = split(rbuf[:, rows, :].reshape(256, 256))
        dh, dl = dth[other], dtl[other]
        o_ref[...] += (
            jnp.dot(dh, high, preferred_element_type=F32)
            + jnp.dot(dl, high, preferred_element_type=F32)
            + jnp.dot(dh, low, preferred_element_type=F32)
        )

    o_ref[...] = jnp.zeros_like(o_ref)
    for number in (15, 1):
        from_z(number)
    for ps in range(4):
        design_slot(0, ps)
    along_y(0)
    for number in (14, 2):
        from_z(number)
    for ps in (3, 2, 1, 0):
        design_slot(1, ps)
        design_slot(3, 3 - ps)
    along_y(1)
    along_y(3)
    for number in (13, 3, 12, 4):
        from_z(number)
    for ps in (1, 2, 0, 3):
        design_slot(2, ps)
    along_y(2)
    for number in DIRECT:
        relay_z(number)
    relay_y(0)
    for number in (0, 15, 1, 14, 2):
        relay_x(number)
    relay_y(1)
    relay_y(3)
    for number in (13, 3, 12, 4):
        relay_x(number)
    last_y(0)
    for number in RELAYED[:2]:
        from_z(number)
    last_y(1)
    relay_y(2)
    last_y(3)
    prepare(0)
    for number in RELAYED[2:4]:
        from_z(number)
    for number in RELAYED[:2]:
        relay_x(number)
    last_y(2)
    prepare(1)
    prepare(3)
    for number in RELAYED[4:6]:
        from_z(number)
    for number in RELAYED[2:4]:
        relay_x(number)
    for number in [0, *DIRECT]:
        last_x(number)
    prepare(2)

    @pl.loop(0, 5)
    def _(slot):
        multiply(slot)

    for number in RELAYED[6:8]:
        from_z(number)
    for number in RELAYED[4:6]:
        relay_x(number)

    @pl.loop(12, 16)
    def _(slot):
        multiply(slot)

    for number in RELAYED[:4]:
        last_x(number)
    for number in RELAYED[6:8]:
        relay_x(number)
    for first in (5, 10):

        @pl.loop(first, first + 2)
        def _(slot):
            multiply(slot)

    for number in RELAYED[4:]:
        last_x(number)

    @pl.loop(7, 10)
    def _(slot):
        multiply(slot)

    for copy, when in started:
        if when is None:
            copy.wait_send()
        else:
            pl.when(when)(copy.wait_send)


def body(design, responses):
    dma = pltpu.SemaphoreType.DMA
    return pl.pallas_call(
        kernel,
        out_shape=jax.ShapeDtypeStruct((512, 256), F32),
        in_specs=[pl.BlockSpec(memory_space=pl.ANY)] * 2,
        out_specs=pl.BlockSpec(memory_space=pltpu.VMEM),
        scratch_shapes=[
            pltpu.VMEM((64, 1024), F32),
            pltpu.VMEM((64, 1024), F32),
            pltpu.VMEM((4, 16, 1024), F32),
            pltpu.VMEM((2, 64, 4, 16, 256), F32),
            pltpu.VMEM((4, 1024, 256), F32),
            pltpu.VMEM((16, 512, 256), BF16),
            pltpu.VMEM((16, 512, 256), BF16),
            dma((3,)),
            dma((142,)),
            dma((16,)),
            dma((4, 4)),
            dma((4, 4)),
            dma((4,)),
            dma((17,)),
            dma((4, 17)),
        ],
        compiler_params=pltpu.CompilerParams(
            collective_id=0, has_side_effects=True, vmem_limit_bytes=60 * 2**20
        ),
    )(design, responses)


def solution(mesh):
    finer = Mesh(
        mesh.devices.reshape(4, 4, 4, 2, 4), ("x", "zh", "y", "c", "p")
    )
    spec = P(("x", "zh", "p"), ("y", "c"))
    return jax.shard_map(
        body,
        mesh=finer,
        in_specs=(spec, spec),
        out_specs=P(("x", "zh"), ("y", "c", "p")),
        check_vma=False,
    )
```

```python
import jax
import jax.numpy as jnp
from jax import lax
from jax.experimental import pallas as pl
from jax.experimental.pallas import tpu as pltpu
from jax.sharding import Mesh
from jax.sharding import PartitionSpec as P

MESH = pl.DeviceIdType.MESH
F32, BF16 = jnp.float32, jnp.bfloat16

X_OWN, Z_SEND, TURNED, D_SEND, D_SLOT, Y_UP, Y_DOWN, Y_LAST = range(8)
R_SLOT, Z_RELAY, X_UP, X_DOWN, X_LAST, PREPARE, MULTIPLY = range(8, 15)
OWN, NEAR, AWAY, FAR = range(4)

EDGE = [
    (Z_SEND, -1), (Z_SEND, 4), (Z_SEND, 3), (Z_SEND, 1), (Z_SEND, -2), (Z_SEND, -4), (Z_SEND, -3), (Z_SEND, 2), (TURNED,),
    (D_SEND,), (D_SLOT, OWN, 0), (R_SLOT, 14), (D_SLOT, NEAR, 1), (R_SLOT, 15), (X_UP, 14), (D_SLOT, NEAR, 0),
    (D_SLOT, NEAR, 2), (R_SLOT, 12), (R_SLOT, 3), (Z_RELAY, 15), (R_SLOT, 2), (R_SLOT, 4), (Z_RELAY, 2), (D_SLOT, NEAR, 3),
    (D_SLOT, FAR, 3), (X_DOWN, 12), (Z_RELAY, 14), (D_SLOT, OWN, 3), (X_DOWN, 4), (X_DOWN, 3), (Y_DOWN, NEAR, 3),
    (R_SLOT, 1), (Y_UP, OWN, 0), (Y_UP, FAR, 3), (Y_UP, NEAR, 3), (D_SLOT, OWN, 2), (Y_DOWN, NEAR, 0), (R_SLOT, 11),
    (Z_RELAY, 4), (X_DOWN, 14), (X_DOWN, 15), (D_SLOT, OWN, 1), (Y_DOWN, NEAR, 1), (Y_DOWN, OWN, 3), (Y_LAST, NEAR, 3),
    (Y_DOWN, OWN, 2), (X_OWN,), (Y_UP, NEAR, 1), (R_SLOT, 13), (X_LAST, 14), (Y_UP, OWN, 2), (D_SLOT, AWAY, 2),
    (R_SLOT, 6), (X_UP, 12), (X_DOWN, 13), (D_SLOT, AWAY, 3), (D_SLOT, FAR, 2), (X_UP, 4), (X_UP, 2), (R_SLOT, 10),
    (Y_LAST, NEAR, 1), (Y_UP, NEAR, 0), (X_UP, 1), (Y_UP, NEAR, 2), (Z_RELAY, 12), (X_UP, 11), (Z_RELAY, 1), (X_UP, 15),
    (Y_UP, OWN, 3), (R_SLOT, 8), (Y_DOWN, OWN, 1), (X_UP, 0), (Y_DOWN, NEAR, 2), (Y_UP, OWN, 1), (X_UP, 13),
    (Y_LAST, OWN, 1), (Y_UP, AWAY, 2), (X_DOWN, 1), (R_SLOT, 16), (X_DOWN, 6), (X_UP, 6), (Y_DOWN, AWAY, 2),
    (Y_DOWN, OWN, 0), (X_DOWN, 11), (D_SLOT, AWAY, 1), (Y_DOWN, AWAY, 3), (D_SLOT, AWAY, 0), (X_LAST, 12), (Z_RELAY, 13),
    (Y_LAST, NEAR, 0), (X_DOWN, 0), (Y_LAST, NEAR, 2), (R_SLOT, 5), (PREPARE, NEAR), (X_LAST, 1), (Y_DOWN, FAR, 2),
    (X_UP, 10), (X_DOWN, 2), (Z_RELAY, 3), (D_SLOT, FAR, 0), (Y_DOWN, AWAY, 0), (Y_LAST, OWN, 2), (X_LAST, 15),
    (X_DOWN, 10), (X_UP, 3), (Y_UP, AWAY, 3), (X_LAST, 13), (Y_UP, FAR, 2), (R_SLOT, 9), (Y_UP, AWAY, 1), (Y_DOWN, FAR, 3),
    (X_UP, 5), (Y_DOWN, AWAY, 1), (X_DOWN, 5), (X_LAST, 0), (Y_UP, AWAY, 0), (X_LAST, 2), (X_LAST, 4), (Y_LAST, AWAY, 2),
    (X_UP, 16), (X_DOWN, 16), (X_LAST, 3), (Y_LAST, OWN, 3), (D_SLOT, FAR, 1), (X_UP, 8), (Y_LAST, AWAY, 3), (X_DOWN, 8),
    (Y_LAST, OWN, 0), (Y_DOWN, FAR, 0), (MULTIPLY, NEAR, 2), (X_LAST, 10), (Y_UP, FAR, 0), (R_SLOT, 7), (PREPARE, OWN),
    (X_UP, 9), (Y_UP, FAR, 1), (Y_DOWN, FAR, 1), (Y_LAST, FAR, 3), (X_DOWN, 9), (MULTIPLY, OWN, 2), (MULTIPLY, OWN, 0),
    (Y_LAST, AWAY, 1), (Y_LAST, FAR, 2), (MULTIPLY, OWN, 3), (Y_LAST, FAR, 0), (Y_LAST, AWAY, 0), (X_LAST, 16),
    (X_LAST, 11), (X_LAST, 6), (X_LAST, 5), (MULTIPLY, NEAR, 0), (MULTIPLY, NEAR, 3), (X_UP, 7), (X_DOWN, 7),
    (MULTIPLY, NEAR, 1), (MULTIPLY, OWN, 1), (Y_LAST, FAR, 1), (X_LAST, 8), (PREPARE, AWAY), (MULTIPLY, AWAY, 0),
    (PREPARE, FAR), (X_LAST, 7), (X_LAST, 9), (MULTIPLY, AWAY, 3), (MULTIPLY, AWAY, 1), (MULTIPLY, FAR, 1),
    (MULTIPLY, FAR, 2), (MULTIPLY, FAR, 3), (MULTIPLY, FAR, 0), (MULTIPLY, AWAY, 2),
]
INNER = [
    (Z_SEND, -1), (Z_SEND, 4), (Z_SEND, -2), (Z_SEND, 3), (Z_SEND, -4), (Z_SEND, 2), (Z_SEND, 1), (Z_SEND, -3), (TURNED,),
    (D_SEND,), (X_OWN,), (D_SLOT, OWN, 1), (D_SLOT, OWN, 0), (D_SLOT, OWN, 2), (R_SLOT, 4), (R_SLOT, 14),
    (D_SLOT, NEAR, 1), (D_SLOT, NEAR, 0), (R_SLOT, 15), (D_SLOT, OWN, 3), (D_SLOT, NEAR, 2), (R_SLOT, 1), (Y_DOWN, OWN, 2),
    (X_DOWN, 0), (D_SLOT, AWAY, 2), (R_SLOT, 2), (D_SLOT, AWAY, 3), (Y_DOWN, OWN, 0), (X_UP, 14), (D_SLOT, NEAR, 3),
    (Z_RELAY, 1), (Y_UP, OWN, 1), (R_SLOT, 13), (Y_UP, OWN, 0), (Y_DOWN, NEAR, 2), (X_DOWN, 2), (Z_RELAY, 2),
    (Y_UP, NEAR, 0), (X_UP, 15), (R_SLOT, 12), (Z_RELAY, 14), (X_DOWN, 15), (R_SLOT, 3), (Y_LAST, OWN, 0), (Y_UP, NEAR, 2),
    (D_SLOT, AWAY, 1), (X_DOWN, 1), (X_UP, 0), (Y_DOWN, NEAR, 0), (Z_RELAY, 15), (X_UP, 3), (Y_UP, OWN, 2), (R_SLOT, 10),
    (D_SLOT, AWAY, 0), (D_SLOT, FAR, 3), (Z_RELAY, 12), (X_DOWN, 12), (Y_DOWN, NEAR, 3), (R_SLOT, 5), (Z_RELAY, 3),
    (Y_DOWN, AWAY, 0), (X_DOWN, 14), (Y_DOWN, AWAY, 2), (Y_UP, NEAR, 3), (Y_UP, AWAY, 0), (X_UP, 1), (X_DOWN, 3),
    (Y_DOWN, OWN, 3), (Y_UP, AWAY, 2), (X_UP, 4), (Y_LAST, NEAR, 0), (X_DOWN, 10), (X_UP, 13), (Y_DOWN, NEAR, 1),
    (X_LAST, 0), (X_DOWN, 4), (Z_RELAY, 4), (X_UP, 5), (D_SLOT, FAR, 0), (R_SLOT, 6), (X_DOWN, 13), (D_SLOT, FAR, 2),
    (X_UP, 12), (Y_UP, AWAY, 1), (R_SLOT, 11), (Y_UP, NEAR, 1), (Y_LAST, AWAY, 2), (X_UP, 6), (Y_DOWN, OWN, 1),
    (Y_UP, AWAY, 3), (Y_LAST, NEAR, 2), (X_LAST, 14), (Y_DOWN, FAR, 0), (R_SLOT, 7), (X_LAST, 1), (Z_RELAY, 13),
    (Y_LAST, OWN, 2), (X_DOWN, 5), (X_LAST, 12), (Y_LAST, NEAR, 3), (D_SLOT, FAR, 1), (R_SLOT, 8), (X_UP, 2),
    (Y_DOWN, AWAY, 3), (X_UP, 10), (R_SLOT, 16), (Y_LAST, NEAR, 1), (Y_UP, OWN, 3), (Y_LAST, OWN, 1), (X_DOWN, 11),
    (X_UP, 7), (X_DOWN, 7), (X_LAST, 3), (Y_DOWN, AWAY, 1), (X_LAST, 4), (Y_LAST, AWAY, 0), (X_LAST, 13), (PREPARE, NEAR),
    (X_LAST, 2), (X_UP, 11), (X_UP, 16), (Y_UP, FAR, 1), (Y_LAST, AWAY, 3), (Y_LAST, OWN, 3), (Y_UP, FAR, 0), (X_DOWN, 6),
    (MULTIPLY, NEAR, 2), (R_SLOT, 9), (X_LAST, 7), (Y_DOWN, FAR, 3), (X_LAST, 15), (X_DOWN, 16), (MULTIPLY, NEAR, 1),
    (X_LAST, 5), (PREPARE, OWN), (Y_DOWN, FAR, 1), (X_UP, 8), (Y_LAST, AWAY, 1), (Y_UP, FAR, 3), (Y_DOWN, FAR, 2),
    (MULTIPLY, OWN, 0), (X_DOWN, 8), (Y_LAST, FAR, 0), (Y_UP, FAR, 2), (X_DOWN, 9), (X_UP, 9), (MULTIPLY, OWN, 3),
    (MULTIPLY, OWN, 1), (X_LAST, 10), (MULTIPLY, NEAR, 3), (X_LAST, 11), (MULTIPLY, OWN, 2), (PREPARE, AWAY),
    (Y_LAST, FAR, 3), (MULTIPLY, AWAY, 0), (X_LAST, 16), (MULTIPLY, AWAY, 1), (X_LAST, 6), (X_LAST, 8), (Y_LAST, FAR, 1),
    (X_LAST, 9), (Y_LAST, FAR, 2), (MULTIPLY, AWAY, 3), (MULTIPLY, AWAY, 2), (MULTIPLY, NEAR, 0), (PREPARE, FAR),
    (MULTIPLY, FAR, 3), (MULTIPLY, FAR, 0), (MULTIPLY, FAR, 2), (MULTIPLY, FAR, 1),
]

PIECES = (
    [(64 * s, 64) for s in range(8)]
    + [(512, 32)]
    + [(64 * s, 64) for s in range(9, 16)]
    + [(544, 32)]
)


def split(value):
    high = value.astype(BF16)
    return high, (value - high.astype(F32)).astype(BF16)


def kernel(d_hbm, r_hbm, o_ref, dv, rv, turned, dbuf, rbuf, dth, dtl, local, ss, tz, dz, dy, dd, rz, rx):
    x, zh, y, c, p = (lax.axis_index(n) for n in ("x", "zh", "y", "c", "p"))
    z = 4 * zh + p

    def ring(v, n):
        return lax.rem(v + 4 * n, n)

    def at_z(d):
        w = ring(z + d, 16)
        return {"zh": lax.div(w, 4), "p": lax.rem(w, 4)}

    up_x, down_x = {"x": ring(x + 1, 4)}, {"x": ring(x - 1, 4)}
    up_y, down_y = {"y": ring(y + 1, 4)}, {"y": ring(y - 1, 4)}
    partner = {"c": 1 - c}
    source_core = lax.div(zh, 2)
    diagonal = x == y
    holder = c == source_core
    low = p < 2

    load_d = pltpu.make_async_copy(d_hbm, dv, local.at[0])
    load_r = pltpu.make_async_copy(r_hbm, rv, local.at[1])
    own = r_hbm.at[:, pl.ds(pl.multiple_of(p * 256, 256), 256)]
    load_own = pltpu.make_async_copy(own, rbuf.at[x, pl.ds(0, 64)], local.at[2])
    load_d.start()
    load_r.start()
    load_own.start()

    barrier = pltpu.get_barrier_semaphore()

    def greet(device, when=None):
        def signal():
            pl.semaphore_signal(barrier, inc=1, device_id=device, device_id_type=MESH)

        if when is None:
            signal()
        else:
            pl.when(when)(signal)

    for d in (1, -1, 2, -2, 3, -3, 4, -4):
        greet(at_z(d))
    for device in (up_x, down_x, up_y, down_y, partner):
        greet(device)
    for other in range(4):
        greet({"x": other, "y": x}, jnp.logical_or(x != other, y != x))
    for r in (1, 3, 2):
        for ps in range(4):
            origin = {"zh": ring(zh - r, 4), "p": ps, "c": source_core}
            upward = r == 1 or (r == 2 and ps >= 2)
            greet(origin, p == (0 if upward else 3))
    o_ref[...] = jnp.zeros_like(o_ref)
    load_d.wait()
    load_own.wait()
    load_r.wait()
    pl.semaphore_wait(
        barrier,
        4 - diagonal.astype(jnp.int32) + 8 + 5 + jnp.where(holder, 2, 4),
    )

    def go(order, inner):
        started = []

        def send(src, dst, sem, device, when=None):
            copy = pltpu.make_async_remote_copy(
                src_ref=src,
                dst_ref=dst,
                send_sem=ss.at[len(started)],
                recv_sem=sem,
                device_id=device,
                device_id_type=MESH,
            )
            started.append((copy, when))
            if when is None:
                copy.start()
            else:
                pl.when(when)(copy.start)

        def arrived(dst, sem, when=None):
            copy = pltpu.make_async_copy(dst, dst, sem)
            if when is None:
                copy.wait()
            else:
                pl.when(when)(copy.wait)

        for part in range(4):
            send(
                dv.at[pl.ds(16 * part, 16)],
                turned.at[x],
                tz.at[x],
                {"x": y, "y": part},
                jnp.logical_or(x != y, y != part),
            )

        @pl.when(diagonal)
        def _():
            turned[x] = dv[pl.ds(pl.multiple_of(16 * y, 16), 16), :]

        def turned_in():
            for other in range(4):
                arrived(
                    turned.at[other],
                    tz.at[other],
                    jnp.logical_or(x != other, y != x),
                )

        def block(core, slot, part, half=None):
            first, count = (4 * slot, 4) if half is None else (4 * slot + 2 * half, 2)
            return dbuf.at[core, pl.ds(first, count), part]

        def d_send():
            for h in range(2):
                target = 2 * c + h
                rel = ring(target - zh, 4)
                up = jnp.logical_or(rel == 1, jnp.logical_and(rel == 2, p >= 2))
                entry = jnp.where(rel == 0, p, jnp.where(up, 0, 3))
                slot = 4 * rel + p
                for core in range(2):
                    columns = pl.ds(512 * h + 256 * core, 256)
                    mine = jnp.logical_and(rel == 0, c == core)
                    send(
                        turned.at[:, :, columns],
                        block(core, slot, y),
                        dz.at[slot],
                        {"zh": target, "p": entry, "c": core},
                        jnp.logical_not(mine),
                    )

                    @pl.when(mine)
                    def _():
                        dbuf[core, pl.ds(4 * p, 4), y] = turned[:, :, columns]

        ahead, behind = at_z(jnp.where(low, 1, -1)), at_z(jnp.where(low, -1, 1))
        group_of = {
            OWN: 0,
            NEAR: jnp.where(low, 1, 3),
            AWAY: jnp.where(low, 3, 1),
            FAR: 2,
        }
        here = 1 if inner else 0

        def slot_of(r, k):
            return 4 * group_of[r] + jnp.where(low, k, 3 - k)

        def d_slot(r, k):
            slot = slot_of(r, k)
            held = block(c, slot, y)
            if r == OWN and k == here:
                arrived(held, dz.at[slot], jnp.logical_not(holder))
            else:
                arrived(held, dz.at[slot])
            if r == OWN:
                goes = (k <= here, k >= here and inner)
            elif r == NEAR or (r == FAR and k >= 2):
                goes = (True, False)
            else:
                goes = (False, inner)
            for wanted, device in zip(goes, (ahead, behind)):
                if wanted:
                    send(held, held, dz.at[slot], device)
            send(held, held, dy.at[0, slot], up_y)
            send(held, held, dy.at[1, slot], down_y)
            to_partner(r, 0)

        y_of = [y, ring(y - 1, 4), ring(y + 1, 4), ring(y + 2, 4)]
        missing = {(r, which): 4 for r in group_of for which in range(4)}

        def whole(core, r, which):
            first = pl.multiple_of(16 * group_of[r], 16)
            return dbuf.at[core, pl.ds(first, 16), y_of[which]]

        def to_partner(r, which):
            missing[r, which] -= 1
            if missing[r, which] == 0:
                part = whole(c, r, which)
                send(part, part, dd.at[group_of[r], which], partner)

        def y_relay(side, r, k):
            slot, part = slot_of(r, k), y_of[1 + side]
            arrived(block(c, slot, part), dy.at[side, slot])
            half = block(c, slot, part, side)
            send(half, half, dy.at[2 + side, slot], (up_y, down_y)[side])
            to_partner(r, 1 + side)

        def y_last(r, k):
            slot = slot_of(r, k)
            for side in range(2):
                arrived(block(c, slot, y_of[3], side), dy.at[2 + side, slot])
            to_partner(r, 3)

        def piece(number, owner, half=None):
            first, count = PIECES[number]
            if half is not None:
                first, count = first + half * (count // 2), count // 2
            return rbuf.at[owner, pl.ds(first, count)]

        def z_send(d):
            quarter = pl.ds(pl.multiple_of(ring(p + d, 4) * 256, 256), 256)
            slot = (-d) % 16
            send(rv.at[:, quarter], piece(slot, x), rz.at[slot], at_z(d))

        def z_relay(number):
            side, cut = (4, 12) if number >= 12 else (-4, 4)
            half = (1 if cut == 12 else 0) if number == cut else None
            there = {12: 16, 4: 8}.get(number, number - side)
            send(piece(number, x, half), piece(there, x), rz.at[there], at_z(side))

        def along_x(number):
            for side, device in ((0, up_x), (1, down_x)):
                send(piece(number, x), piece(number, x), rx.at[side, number], device)

        def r_slot(number):
            arrived(piece(number, x), rz.at[number])
            along_x(number)

        x_of = [ring(x - 1, 4), ring(x + 1, 4), ring(x + 2, 4)]

        def x_relay(side, number):
            arrived(piece(number, x_of[side]), rx.at[side, number])
            half = piece(number, x_of[side], side)
            send(half, half, rx.at[2 + side, number], (up_x, down_x)[side])

        def x_last(number):
            for side in range(2):
                arrived(piece(number, x_of[2], side), rx.at[2 + side, number])

        def prepare(r):
            for which in range(4):
                arrived(whole(1 - c, r, which), dd.at[group_of[r], which])

            @pl.loop(0, 4)
            def _(ps):
                slot = 4 * group_of[r] + ps
                for half in range(2):
                    value = dbuf[half, pl.ds(4 * slot, 4)].reshape(256, 256).T
                    high, rest = split(value)
                    dth[slot, pl.ds(256 * half, 256), :] = high
                    dtl[slot, pl.ds(256 * half, 256), :] = rest

        def multiply(r, k):
            slot = slot_of(r, k)
            there = ring(jnp.where(low, k, 3 - k) - p - 4 * group_of[r], 16)
            rows = pl.ds(pl.multiple_of(64 * there, 64), 64)
            high, rest = split(rbuf[:, rows, :].reshape(256, 256))
            dh, dl = dth[slot], dtl[slot]
            o_ref[...] += (
                jnp.dot(dh, high, preferred_element_type=F32)
                + jnp.dot(dl, high, preferred_element_type=F32)
                + jnp.dot(dh, rest, preferred_element_type=F32)
            )

        steps = {
            X_OWN: lambda: along_x(0),
            Z_SEND: z_send,
            TURNED: turned_in,
            D_SEND: d_send,
            D_SLOT: d_slot,
            Y_UP: lambda r, k: y_relay(0, r, k),
            Y_DOWN: lambda r, k: y_relay(1, r, k),
            Y_LAST: y_last,
            R_SLOT: r_slot,
            Z_RELAY: z_relay,
            X_UP: lambda number: x_relay(0, number),
            X_DOWN: lambda number: x_relay(1, number),
            X_LAST: x_last,
            PREPARE: prepare,
            MULTIPLY: multiply,
        }
        for name, *numbers in order:
            steps[name](*numbers)
        for copy, when in started:
            if when is None:
                copy.wait_send()
            else:
                pl.when(when)(copy.wait_send)

    edge = jnp.logical_or(p == 0, p == 3)
    pl.when(edge)(lambda: go(EDGE, False))
    pl.when(jnp.logical_not(edge))(lambda: go(INNER, True))


def body(design, responses):
    dma = pltpu.SemaphoreType.DMA
    held = [pltpu.with_memory_space_constraint(v, pltpu.HBM) for v in (design, responses)]
    return pl.pallas_call(
        kernel,
        out_shape=jax.ShapeDtypeStruct((512, 256), F32),
        in_specs=[pl.BlockSpec(memory_space=pltpu.HBM)] * 2,
        out_specs=pl.BlockSpec(memory_space=pltpu.VMEM),
        scratch_shapes=[
            pltpu.VMEM((64, 1024), F32),
            pltpu.VMEM((64, 1024), F32),
            pltpu.VMEM((4, 16, 1024), F32),
            pltpu.VMEM((2, 64, 4, 16, 256), F32),
            pltpu.VMEM((4, 1024, 256), F32),
            pltpu.VMEM((16, 512, 256), BF16),
            pltpu.VMEM((16, 512, 256), BF16),
            dma((3,)),
            dma((200,)),
            dma((4,)),
            dma((16,)),
            dma((4, 16)),
            dma((4, 4)),
            dma((17,)),
            dma((4, 17)),
        ],
        compiler_params=pltpu.CompilerParams(
            collective_id=0, has_side_effects=True, vmem_limit_bytes=32 * 2**20
        ),
    )(*held)


def solution(mesh):
    finer = Mesh(
        mesh.devices.reshape(4, 4, 4, 2, 4), ("x", "zh", "y", "c", "p")
    )
    spec = P(("x", "zh", "p"), ("y", "c"))
    return jax.shard_map(
        body,
        mesh=finer,
        in_specs=(spec, spec),
        out_specs=P(("x", "zh"), ("y", "c", "p")),
        check_vma=False,
    )
```

```python
import jax
import jax.numpy as jnp
from jax import lax
from jax.experimental import pallas as pl
from jax.experimental.pallas import tpu as pltpu
from jax.sharding import Mesh
from jax.sharding import PartitionSpec as P

MESH = pl.DeviceIdType.MESH
F32, BF16 = jnp.float32, jnp.bfloat16

X_OWN, Z_SEND, TURNED, D_SEND, D_SLOT, Y_UP, Y_DOWN, Y_LAST = range(8)
R_SLOT, Z_RELAY, X_UP, X_DOWN, X_LAST, PREPARE, MULTIPLY = range(8, 15)
OWN, NEAR, AWAY, FAR = range(4)

EDGE = [
    (Z_SEND, -1), (Z_SEND, 4), (Z_SEND, 3), (Z_SEND, -2), (Z_SEND, 2), (Z_SEND, 1), (Z_SEND, -4), (Z_SEND, -3), (TURNED,),
    (D_SEND,), (R_SLOT, 3), (D_SLOT, OWN, 0), (R_SLOT, 1), (D_SLOT, NEAR, 1), (R_SLOT, 15), (R_SLOT, 2), (R_SLOT, 12),
    (R_SLOT, 14), (X_UP, 1), (D_SLOT, NEAR, 0), (R_SLOT, 4), (D_SLOT, NEAR, 3), (Z_RELAY, 4), (D_SLOT, NEAR, 2),
    (D_SLOT, FAR, 3), (Z_RELAY, 15), (Z_RELAY, 14), (Y_UP, NEAR, 1), (Y_UP, NEAR, 2), (X_UP, 14), (Y_DOWN, NEAR, 2),
    (X_DOWN, 1), (X_UP, 12), (Z_RELAY, 2), (X_UP, 2), (Y_DOWN, OWN, 0), (D_SLOT, OWN, 2), (X_DOWN, 4), (Y_LAST, NEAR, 2),
    (Y_DOWN, NEAR, 1), (X_DOWN, 2), (D_SLOT, AWAY, 2), (Y_DOWN, OWN, 2), (X_LAST, 1), (R_SLOT, 8), (R_SLOT, 6),
    (Y_DOWN, FAR, 3), (Y_UP, NEAR, 0), (X_DOWN, 12), (D_SLOT, FAR, 2), (D_SLOT, OWN, 3), (X_OWN,), (R_SLOT, 11),
    (Y_UP, AWAY, 2), (X_UP, 8), (Y_UP, NEAR, 3), (Y_DOWN, AWAY, 2), (X_DOWN, 14), (Y_UP, OWN, 2), (R_SLOT, 13),
    (R_SLOT, 10), (Y_UP, FAR, 3), (X_UP, 3), (Y_DOWN, NEAR, 3), (D_SLOT, OWN, 1), (Z_RELAY, 12), (X_DOWN, 0), (X_DOWN, 3),
    (D_SLOT, AWAY, 3), (Z_RELAY, 13), (Y_DOWN, NEAR, 0), (Y_UP, OWN, 1), (X_LAST, 14), (Y_UP, FAR, 2), (X_DOWN, 6),
    (X_UP, 11), (R_SLOT, 16), (D_SLOT, AWAY, 0), (Y_LAST, NEAR, 3), (X_DOWN, 13), (X_UP, 0), (X_UP, 10), (X_DOWN, 11),
    (X_UP, 4), (Y_DOWN, OWN, 3), (X_DOWN, 8), (X_UP, 6), (X_UP, 13), (Y_UP, OWN, 0), (Y_LAST, NEAR, 0), (Y_DOWN, OWN, 1),
    (X_DOWN, 15), (Y_UP, OWN, 3), (Z_RELAY, 1), (X_LAST, 12), (Y_DOWN, AWAY, 3), (Y_LAST, NEAR, 1), (PREPARE, NEAR),
    (Z_RELAY, 3), (X_LAST, 3), (X_UP, 15), (X_LAST, 2), (X_DOWN, 10), (Y_DOWN, FAR, 2), (D_SLOT, AWAY, 1),
    (Y_LAST, OWN, 1), (Y_LAST, OWN, 2), (Y_UP, AWAY, 0), (D_SLOT, FAR, 0), (Y_UP, AWAY, 3), (X_LAST, 0), (R_SLOT, 5),
    (Y_LAST, FAR, 3), (Y_LAST, OWN, 0), (Y_LAST, FAR, 2), (X_UP, 16), (Y_DOWN, AWAY, 1), (X_DOWN, 16), (Y_LAST, AWAY, 2),
    (R_SLOT, 9), (Y_DOWN, AWAY, 0), (X_LAST, 15), (D_SLOT, FAR, 1), (Y_LAST, OWN, 3), (X_LAST, 13), (MULTIPLY, NEAR, 3),
    (Y_UP, FAR, 0), (Y_UP, AWAY, 1), (Y_DOWN, FAR, 0), (X_LAST, 11), (X_DOWN, 5), (X_LAST, 6), (X_UP, 5), (R_SLOT, 7),
    (PREPARE, OWN), (MULTIPLY, OWN, 3), (Y_LAST, AWAY, 3), (Y_LAST, AWAY, 0), (MULTIPLY, OWN, 0), (Y_DOWN, FAR, 1),
    (Y_UP, FAR, 1), (MULTIPLY, OWN, 1), (Y_LAST, FAR, 0), (X_LAST, 8), (Y_LAST, AWAY, 1), (MULTIPLY, OWN, 2), (X_UP, 7),
    (X_DOWN, 9), (X_LAST, 5), (PREPARE, AWAY), (X_UP, 9), (X_LAST, 4), (X_DOWN, 7), (MULTIPLY, AWAY, 0),
    (MULTIPLY, AWAY, 1), (Y_LAST, FAR, 1), (X_LAST, 10), (MULTIPLY, NEAR, 2), (MULTIPLY, AWAY, 2), (MULTIPLY, NEAR, 0),
    (PREPARE, FAR), (MULTIPLY, FAR, 3), (MULTIPLY, NEAR, 1), (X_LAST, 9), (X_LAST, 7), (X_LAST, 16), (MULTIPLY, FAR, 2),
    (MULTIPLY, AWAY, 3), (MULTIPLY, FAR, 0), (MULTIPLY, FAR, 1),
]
INNER = [
    (Z_SEND, 4), (Z_SEND, 3), (Z_SEND, -1), (Z_SEND, -2), (Z_SEND, 1), (Z_SEND, 2), (Z_SEND, -4), (Z_SEND, -3), (TURNED,),
    (D_SEND,), (R_SLOT, 14), (R_SLOT, 1), (D_SLOT, OWN, 1), (X_UP, 1), (D_SLOT, OWN, 2), (R_SLOT, 15), (D_SLOT, OWN, 0),
    (D_SLOT, NEAR, 1), (R_SLOT, 12), (D_SLOT, NEAR, 0), (Y_DOWN, OWN, 2), (D_SLOT, NEAR, 3), (Y_UP, OWN, 0),
    (D_SLOT, OWN, 3), (R_SLOT, 3), (Y_DOWN, OWN, 1), (Y_UP, OWN, 2), (R_SLOT, 4), (R_SLOT, 2), (X_DOWN, 12),
    (D_SLOT, AWAY, 2), (X_UP, 12), (X_DOWN, 1), (X_UP, 4), (Y_DOWN, NEAR, 0), (X_DOWN, 14), (D_SLOT, NEAR, 2), (X_DOWN, 3),
    (Z_RELAY, 2), (Z_RELAY, 1), (X_OWN,), (Z_RELAY, 14), (D_SLOT, AWAY, 3), (Z_RELAY, 3), (X_UP, 14), (Y_UP, NEAR, 0),
    (Y_DOWN, NEAR, 2), (X_DOWN, 4), (R_SLOT, 13), (X_DOWN, 0), (Y_UP, NEAR, 2), (Z_RELAY, 15), (Y_DOWN, OWN, 3),
    (Y_DOWN, AWAY, 3), (D_SLOT, FAR, 3), (R_SLOT, 6), (X_LAST, 1), (Y_LAST, NEAR, 2), (D_SLOT, AWAY, 0), (Y_UP, OWN, 1),
    (X_DOWN, 2), (D_SLOT, AWAY, 1), (R_SLOT, 5), (D_SLOT, FAR, 2), (Z_RELAY, 4), (Y_DOWN, OWN, 0), (Y_UP, OWN, 3),
    (Z_RELAY, 12), (X_UP, 13), (Y_DOWN, AWAY, 0), (X_UP, 15), (Y_UP, AWAY, 0), (X_UP, 3), (Y_DOWN, NEAR, 3),
    (D_SLOT, FAR, 0), (Y_DOWN, FAR, 3), (R_SLOT, 11), (X_UP, 6), (Y_UP, AWAY, 1), (Y_UP, FAR, 3), (Y_DOWN, FAR, 2),
    (Y_UP, NEAR, 1), (Y_UP, NEAR, 3), (X_LAST, 12), (Z_RELAY, 13), (Y_DOWN, NEAR, 1), (X_UP, 2), (R_SLOT, 10),
    (X_DOWN, 15), (R_SLOT, 7), (Y_UP, FAR, 2), (Y_DOWN, FAR, 0), (X_DOWN, 13), (R_SLOT, 8), (D_SLOT, FAR, 1),
    (Y_DOWN, AWAY, 1), (X_UP, 11), (X_DOWN, 5), (Y_LAST, OWN, 1), (X_UP, 0), (X_DOWN, 11), (X_LAST, 4), (Y_UP, FAR, 0),
    (Y_UP, AWAY, 3), (Y_LAST, OWN, 3), (Y_LAST, FAR, 3), (Y_LAST, NEAR, 1), (Y_DOWN, AWAY, 2), (X_DOWN, 6),
    (Y_LAST, FAR, 0), (X_DOWN, 7), (R_SLOT, 16), (X_UP, 10), (Y_LAST, OWN, 0), (X_LAST, 13), (Y_DOWN, FAR, 1), (X_UP, 8),
    (Y_UP, AWAY, 2), (Y_LAST, OWN, 2), (Y_LAST, AWAY, 0), (Y_UP, FAR, 1), (R_SLOT, 9), (X_LAST, 15), (Y_LAST, AWAY, 1),
    (Y_LAST, NEAR, 3), (PREPARE, OWN), (X_LAST, 2), (X_LAST, 11), (X_LAST, 3), (X_UP, 5), (Y_LAST, FAR, 2), (X_LAST, 0),
    (X_UP, 7), (Y_LAST, NEAR, 0), (X_DOWN, 10), (Y_LAST, AWAY, 2), (Y_LAST, AWAY, 3), (X_LAST, 14), (MULTIPLY, OWN, 2),
    (PREPARE, NEAR), (Y_LAST, FAR, 1), (MULTIPLY, OWN, 3), (X_UP, 9), (X_DOWN, 8), (X_UP, 16), (X_DOWN, 9),
    (MULTIPLY, NEAR, 2), (MULTIPLY, NEAR, 1), (X_DOWN, 16), (X_LAST, 5), (PREPARE, AWAY), (PREPARE, FAR), (X_LAST, 10),
    (MULTIPLY, AWAY, 0), (X_LAST, 7), (MULTIPLY, NEAR, 0), (X_LAST, 8), (X_LAST, 6), (MULTIPLY, OWN, 1), (X_LAST, 9),
    (MULTIPLY, AWAY, 2), (X_LAST, 16), (MULTIPLY, FAR, 0), (MULTIPLY, FAR, 3), (MULTIPLY, AWAY, 3), (MULTIPLY, FAR, 1),
    (MULTIPLY, OWN, 0), (MULTIPLY, NEAR, 3), (MULTIPLY, AWAY, 1), (MULTIPLY, FAR, 2),
]

PIECES = (
    [(64 * s, 64) for s in range(8)]
    + [(512, 32)]
    + [(64 * s, 64) for s in range(9, 16)]
    + [(544, 32)]
)


def split(value):
    high = value.astype(BF16)
    return high, (value - high.astype(F32)).astype(BF16)


def kernel(d_hbm, r_hbm, o_ref, dv, rv, turned, dbuf, rbuf, dth, dtl, local, ss, tz, dz, dy, dd, rz, rx):
    x, zh, y, c, p = (lax.axis_index(n) for n in ("x", "zh", "y", "c", "p"))
    z = 4 * zh + p

    def ring(v, n):
        return lax.rem(v + 4 * n, n)

    def at_z(d):
        w = ring(z + d, 16)
        return {"zh": lax.div(w, 4), "p": lax.rem(w, 4)}

    up_x, down_x = {"x": ring(x + 1, 4)}, {"x": ring(x - 1, 4)}
    up_y, down_y = {"y": ring(y + 1, 4)}, {"y": ring(y - 1, 4)}
    partner = {"c": 1 - c}
    source_core = lax.div(zh, 2)
    diagonal = x == y
    holder = c == source_core
    low = p < 2

    load_d = pltpu.make_async_copy(d_hbm, dv, local.at[0])
    load_r = pltpu.make_async_copy(r_hbm, rv, local.at[1])
    own = r_hbm.at[:, pl.ds(pl.multiple_of(p * 256, 256), 256)]
    load_own = pltpu.make_async_copy(own, rbuf.at[x, pl.ds(0, 64)], local.at[2])
    load_d.start()
    load_r.start()
    load_own.start()

    barrier = pltpu.get_barrier_semaphore()

    def greet(device, when=None):
        def signal():
            pl.semaphore_signal(barrier, inc=1, device_id=device, device_id_type=MESH)

        if when is None:
            signal()
        else:
            pl.when(when)(signal)

    for d in (1, -1, 2, -2, 3, -3, 4, -4):
        greet(at_z(d))
    for device in (up_x, down_x, up_y, down_y, partner):
        greet(device)
    for other in range(4):
        greet({"x": other, "y": x}, jnp.logical_or(x != other, y != x))
    for r in (1, 3, 2):
        for ps in range(4):
            origin = {"zh": ring(zh - r, 4), "p": ps, "c": source_core}
            upward = r == 1 or (r == 2 and ps >= 2)
            greet(origin, p == (0 if upward else 3))
    o_ref[...] = jnp.zeros_like(o_ref)
    load_d.wait()
    load_own.wait()
    load_r.wait()
    pl.semaphore_wait(
        barrier,
        4 - diagonal.astype(jnp.int32) + 8 + 5 + jnp.where(holder, 2, 4),
    )

    def go(order, inner):
        started = []

        def send(src, dst, sem, device, when=None):
            copy = pltpu.make_async_remote_copy(
                src_ref=src,
                dst_ref=dst,
                send_sem=ss.at[len(started)],
                recv_sem=sem,
                device_id=device,
                device_id_type=MESH,
            )
            started.append((copy, when))
            if when is None:
                copy.start()
            else:
                pl.when(when)(copy.start)

        def arrived(dst, sem, when=None):
            copy = pltpu.make_async_copy(dst, dst, sem)
            if when is None:
                copy.wait()
            else:
                pl.when(when)(copy.wait)

        for part in range(4):
            send(
                dv.at[pl.ds(16 * part, 16)],
                turned.at[x],
                tz.at[x],
                {"x": y, "y": part},
                jnp.logical_or(x != y, y != part),
            )

        @pl.when(diagonal)
        def _():
            turned[x] = dv[pl.ds(pl.multiple_of(16 * y, 16), 16), :]

        def turned_in():
            for other in range(4):
                arrived(
                    turned.at[other],
                    tz.at[other],
                    jnp.logical_or(x != other, y != x),
                )

        def block(core, slot, part, half=None):
            first, count = (4 * slot, 4) if half is None else (4 * slot + 2 * half, 2)
            return dbuf.at[core, pl.ds(first, count), part]

        def d_send():
            for h in range(2):
                target = 2 * c + h
                rel = ring(target - zh, 4)
                up = jnp.logical_or(rel == 1, jnp.logical_and(rel == 2, p >= 2))
                entry = jnp.where(rel == 0, p, jnp.where(up, 0, 3))
                slot = 4 * rel + p
                for core in range(2):
                    columns = pl.ds(512 * h + 256 * core, 256)
                    mine = jnp.logical_and(rel == 0, c == core)
                    send(
                        turned.at[:, :, columns],
                        block(core, slot, y),
                        dz.at[slot],
                        {"zh": target, "p": entry, "c": core},
                        jnp.logical_not(mine),
                    )

                    @pl.when(mine)
                    def _():
                        dbuf[core, pl.ds(4 * p, 4), y] = turned[:, :, columns]

        ahead, behind = at_z(jnp.where(low, 1, -1)), at_z(jnp.where(low, -1, 1))
        group_of = {
            OWN: 0,
            NEAR: jnp.where(low, 1, 3),
            AWAY: jnp.where(low, 3, 1),
            FAR: 2,
        }
        here = 1 if inner else 0

        def slot_of(r, k):
            return 4 * group_of[r] + jnp.where(low, k, 3 - k)

        def d_slot(r, k):
            slot = slot_of(r, k)
            held = block(c, slot, y)
            if r == OWN and k == here:
                arrived(held, dz.at[slot], jnp.logical_not(holder))
            else:
                arrived(held, dz.at[slot])
            if r == OWN:
                goes = (k <= here, k >= here and inner)
            elif r == NEAR or (r == FAR and k >= 2):
                goes = (True, False)
            else:
                goes = (False, inner)
            for wanted, device in zip(goes, (ahead, behind)):
                if wanted:
                    send(held, held, dz.at[slot], device)
            send(held, held, dy.at[0, slot], up_y)
            send(held, held, dy.at[1, slot], down_y)
            to_partner(r, 0)

        y_of = [y, ring(y - 1, 4), ring(y + 1, 4), ring(y + 2, 4)]
        missing = {(r, which): 4 for r in group_of for which in range(4)}

        def whole(core, r, which):
            first = pl.multiple_of(16 * group_of[r], 16)
            return dbuf.at[core, pl.ds(first, 16), y_of[which]]

        def to_partner(r, which):
            missing[r, which] -= 1
            if missing[r, which] == 0:
                part = whole(c, r, which)
                send(part, part, dd.at[group_of[r], which], partner)

        def y_relay(side, r, k):
            slot, part = slot_of(r, k), y_of[1 + side]
            arrived(block(c, slot, part), dy.at[side, slot])
            half = block(c, slot, part, side)
            send(half, half, dy.at[2 + side, slot], (up_y, down_y)[side])
            to_partner(r, 1 + side)

        def y_last(r, k):
            slot = slot_of(r, k)
            for side in range(2):
                arrived(block(c, slot, y_of[3], side), dy.at[2 + side, slot])
            to_partner(r, 3)

        def piece(number, owner, half=None):
            first, count = PIECES[number]
            if half is not None:
                first, count = first + half * (count // 2), count // 2
            return rbuf.at[owner, pl.ds(first, count)]

        def z_send(d):
            quarter = pl.ds(pl.multiple_of(ring(p + d, 4) * 256, 256), 256)
            slot = (-d) % 16
            send(rv.at[:, quarter], piece(slot, x), rz.at[slot], at_z(d))

        def z_relay(number):
            side, cut = (4, 12) if number >= 12 else (-4, 4)
            half = (1 if cut == 12 else 0) if number == cut else None
            there = {12: 16, 4: 8}.get(number, number - side)
            send(piece(number, x, half), piece(there, x), rz.at[there], at_z(side))

        def along_x(number):
            for side, device in ((0, up_x), (1, down_x)):
                send(piece(number, x), piece(number, x), rx.at[side, number], device)

        def r_slot(number):
            arrived(piece(number, x), rz.at[number])
            along_x(number)

        x_of = [ring(x - 1, 4), ring(x + 1, 4), ring(x + 2, 4)]

        def x_relay(side, number):
            arrived(piece(number, x_of[side]), rx.at[side, number])
            half = piece(number, x_of[side], side)
            send(half, half, rx.at[2 + side, number], (up_x, down_x)[side])

        def x_last(number):
            for side in range(2):
                arrived(piece(number, x_of[2], side), rx.at[2 + side, number])

        def prepare(r):
            for which in range(4):
                arrived(whole(1 - c, r, which), dd.at[group_of[r], which])

            @pl.loop(0, 4)
            def _(ps):
                slot = 4 * group_of[r] + ps
                for half in range(2):
                    value = dbuf[half, pl.ds(4 * slot, 4)].reshape(256, 256).T
                    high, rest = split(value)
                    dth[slot, pl.ds(256 * half, 256), :] = high
                    dtl[slot, pl.ds(256 * half, 256), :] = rest

        def multiply(r, k):
            slot = slot_of(r, k)
            there = ring(jnp.where(low, k, 3 - k) - p - 4 * group_of[r], 16)
            rows = pl.ds(pl.multiple_of(64 * there, 64), 64)
            high, rest = split(rbuf[:, rows, :].reshape(256, 256))
            dh, dl = dth[slot], dtl[slot]
            o_ref[...] += (
                jnp.dot(dh, high, preferred_element_type=F32)
                + jnp.dot(dl, high, preferred_element_type=F32)
                + jnp.dot(dh, rest, preferred_element_type=F32)
            )

        steps = {
            X_OWN: lambda: along_x(0),
            Z_SEND: z_send,
            TURNED: turned_in,
            D_SEND: d_send,
            D_SLOT: d_slot,
            Y_UP: lambda r, k: y_relay(0, r, k),
            Y_DOWN: lambda r, k: y_relay(1, r, k),
            Y_LAST: y_last,
            R_SLOT: r_slot,
            Z_RELAY: z_relay,
            X_UP: lambda number: x_relay(0, number),
            X_DOWN: lambda number: x_relay(1, number),
            X_LAST: x_last,
            PREPARE: prepare,
            MULTIPLY: multiply,
        }
        for name, *numbers in order:
            steps[name](*numbers)
        for copy, when in started:
            if when is None:
                copy.wait_send()
            else:
                pl.when(when)(copy.wait_send)

    edge = jnp.logical_or(p == 0, p == 3)
    pl.when(edge)(lambda: go(EDGE, False))
    pl.when(jnp.logical_not(edge))(lambda: go(INNER, True))


def body(design, responses):
    dma = pltpu.SemaphoreType.DMA
    held = [pltpu.with_memory_space_constraint(v, pltpu.HBM) for v in (design, responses)]
    return pl.pallas_call(
        kernel,
        out_shape=jax.ShapeDtypeStruct((512, 256), F32),
        in_specs=[pl.BlockSpec(memory_space=pltpu.HBM)] * 2,
        out_specs=pl.BlockSpec(memory_space=pltpu.VMEM),
        scratch_shapes=[
            pltpu.VMEM((64, 1024), F32),
            pltpu.VMEM((64, 1024), F32),
            pltpu.VMEM((4, 16, 1024), F32),
            pltpu.VMEM((2, 64, 4, 16, 256), F32),
            pltpu.VMEM((4, 1024, 256), F32),
            pltpu.VMEM((16, 512, 256), BF16),
            pltpu.VMEM((16, 512, 256), BF16),
            dma((3,)),
            dma((200,)),
            dma((4,)),
            dma((16,)),
            dma((4, 16)),
            dma((4, 4)),
            dma((17,)),
            dma((4, 17)),
        ],
        compiler_params=pltpu.CompilerParams(
            collective_id=0, has_side_effects=True, vmem_limit_bytes=32 * 2**20
        ),
    )(*held)


def solution(mesh):
    finer = Mesh(
        mesh.devices.reshape(4, 4, 4, 2, 4), ("x", "zh", "y", "c", "p")
    )
    spec = P(("x", "zh", "p"), ("y", "c"))
    return jax.shard_map(
        body,
        mesh=finer,
        in_specs=(spec, spec),
        out_specs=P(("x", "zh"), ("y", "c", "p")),
        check_vma=False,
    )
```

```python
import jax
import jax.numpy as jnp
from jax import lax
from jax.experimental import pallas as pl
from jax.experimental.pallas import tpu as pltpu
from jax.sharding import Mesh
from jax.sharding import PartitionSpec as P

MESH = pl.DeviceIdType.MESH
F32, BF16 = jnp.float32, jnp.bfloat16

X_OWN, Z_SEND, TURNED, D_SEND, D_SLOT, Y_UP, Y_DOWN, Y_LAST = range(8)
R_SLOT, Z_RELAY, X_UP, X_DOWN, X_LAST, PREPARE, MULTIPLY = range(8, 15)
OWN, NEAR, AWAY, FAR = range(4)

EDGE = [
    (Z_SEND, 4), (Z_SEND, 3), (Z_SEND, -1), (Z_SEND, 1), (Z_SEND, -2), (Z_SEND, -4), (Z_SEND, 2), (Z_SEND, -3), (TURNED,),
    (D_SEND,), (R_SLOT, 12), (D_SLOT, OWN, 0), (R_SLOT, 1), (X_DOWN, 12), (X_UP, 12), (D_SLOT, NEAR, 1), (R_SLOT, 14),
    (D_SLOT, NEAR, 0), (Y_UP, NEAR, 1), (R_SLOT, 13), (D_SLOT, NEAR, 3), (R_SLOT, 4), (D_SLOT, NEAR, 2), (X_DOWN, 1),
    (Y_UP, NEAR, 0), (R_SLOT, 15), (R_SLOT, 2), (Z_RELAY, 15), (Z_RELAY, 4), (Z_RELAY, 14), (R_SLOT, 3), (X_UP, 15),
    (D_SLOT, FAR, 3), (X_OWN,), (Z_RELAY, 2), (Y_UP, NEAR, 2), (Y_DOWN, NEAR, 0), (Y_DOWN, NEAR, 2), (D_SLOT, OWN, 3),
    (X_DOWN, 15), (D_SLOT, OWN, 2), (X_UP, 3), (D_SLOT, FAR, 2), (X_DOWN, 14), (R_SLOT, 6), (D_SLOT, AWAY, 2),
    (Y_LAST, NEAR, 2), (Y_UP, FAR, 2), (R_SLOT, 10), (Y_DOWN, OWN, 0), (Y_UP, OWN, 2), (R_SLOT, 8), (X_UP, 6),
    (Y_DOWN, NEAR, 3), (R_SLOT, 11), (Y_UP, OWN, 0), (Y_UP, AWAY, 2), (Z_RELAY, 12), (Y_DOWN, AWAY, 2), (Y_UP, NEAR, 3),
    (D_SLOT, OWN, 1), (Y_DOWN, OWN, 2), (Y_UP, FAR, 3), (Y_DOWN, NEAR, 1), (Y_DOWN, FAR, 3), (X_UP, 4), (Y_LAST, NEAR, 0),
    (X_DOWN, 3), (X_UP, 11), (R_SLOT, 16), (Y_LAST, NEAR, 3), (Z_RELAY, 13), (X_UP, 0), (Y_LAST, NEAR, 1), (X_DOWN, 11),
    (Y_UP, OWN, 3), (X_DOWN, 0), (X_DOWN, 10), (Y_LAST, OWN, 0), (X_UP, 1), (Y_DOWN, OWN, 1), (X_UP, 2), (Y_LAST, OWN, 2),
    (D_SLOT, AWAY, 3), (X_DOWN, 6), (Y_DOWN, FAR, 2), (X_UP, 10), (Y_DOWN, OWN, 3), (D_SLOT, AWAY, 0), (Z_RELAY, 1),
    (X_DOWN, 13), (X_UP, 13), (D_SLOT, AWAY, 1), (X_DOWN, 2), (X_LAST, 3), (X_DOWN, 8), (X_UP, 8), (X_LAST, 12),
    (Y_UP, AWAY, 0), (X_LAST, 0), (PREPARE, NEAR), (Z_RELAY, 3), (X_LAST, 2), (X_LAST, 8), (X_LAST, 11), (X_UP, 16),
    (Y_DOWN, AWAY, 3), (Y_DOWN, AWAY, 0), (Y_LAST, AWAY, 2), (X_DOWN, 16), (R_SLOT, 5), (Y_UP, OWN, 1), (Y_UP, AWAY, 3),
    (X_LAST, 15), (X_UP, 14), (D_SLOT, FAR, 0), (R_SLOT, 9), (Y_DOWN, AWAY, 1), (Y_UP, AWAY, 1), (D_SLOT, FAR, 1),
    (Y_DOWN, FAR, 0), (X_LAST, 14), (Y_LAST, OWN, 1), (R_SLOT, 7), (Y_LAST, AWAY, 3), (Y_LAST, OWN, 3), (X_LAST, 10),
    (X_LAST, 6), (X_LAST, 16), (X_LAST, 1), (X_UP, 5), (Y_UP, FAR, 0), (X_DOWN, 5), (X_DOWN, 4), (MULTIPLY, NEAR, 3),
    (X_DOWN, 9), (Y_LAST, AWAY, 1), (X_UP, 9), (Y_LAST, AWAY, 0), (Y_LAST, FAR, 2), (PREPARE, OWN), (Y_LAST, FAR, 3),
    (Y_UP, FAR, 1), (Y_DOWN, FAR, 1), (MULTIPLY, OWN, 0), (PREPARE, AWAY), (X_LAST, 13), (MULTIPLY, OWN, 2), (X_LAST, 4),
    (X_UP, 7), (X_LAST, 5), (X_DOWN, 7), (MULTIPLY, NEAR, 2), (MULTIPLY, NEAR, 1), (MULTIPLY, NEAR, 0), (Y_LAST, FAR, 0),
    (MULTIPLY, AWAY, 2), (X_LAST, 9), (Y_LAST, FAR, 1), (MULTIPLY, OWN, 1), (MULTIPLY, AWAY, 0), (MULTIPLY, OWN, 3),
    (PREPARE, FAR), (X_LAST, 7), (MULTIPLY, FAR, 3), (MULTIPLY, AWAY, 1), (MULTIPLY, FAR, 1), (MULTIPLY, AWAY, 3),
    (MULTIPLY, FAR, 0), (MULTIPLY, FAR, 2),
]
INNER = [
    (Z_SEND, 4), (Z_SEND, 3), (Z_SEND, -1), (Z_SEND, -2), (Z_SEND, -4), (Z_SEND, 1), (Z_SEND, 2), (Z_SEND, -3), (TURNED,),
    (D_SEND,), (D_SLOT, OWN, 1), (D_SLOT, OWN, 2), (D_SLOT, OWN, 0), (R_SLOT, 12), (D_SLOT, NEAR, 1), (R_SLOT, 2),
    (R_SLOT, 14), (R_SLOT, 13), (X_DOWN, 12), (D_SLOT, NEAR, 0), (D_SLOT, OWN, 3), (R_SLOT, 1), (Z_RELAY, 14),
    (D_SLOT, NEAR, 3), (X_UP, 14), (R_SLOT, 4), (D_SLOT, AWAY, 2), (D_SLOT, NEAR, 2), (R_SLOT, 3), (Z_RELAY, 2),
    (Y_DOWN, OWN, 3), (Y_DOWN, OWN, 0), (D_SLOT, AWAY, 3), (X_DOWN, 14), (Z_RELAY, 1), (X_UP, 4), (Y_DOWN, NEAR, 2),
    (X_OWN,), (Y_UP, OWN, 2), (D_SLOT, AWAY, 0), (Y_DOWN, NEAR, 0), (D_SLOT, FAR, 3), (R_SLOT, 15), (Y_DOWN, OWN, 1),
    (Y_UP, NEAR, 0), (X_DOWN, 13), (Y_DOWN, NEAR, 1), (X_DOWN, 0), (Y_UP, OWN, 1), (X_UP, 12), (R_SLOT, 6), (X_UP, 2),
    (Y_UP, NEAR, 3), (Z_RELAY, 15), (Z_RELAY, 3), (Y_UP, OWN, 0), (Y_UP, NEAR, 2), (Y_DOWN, OWN, 2), (X_UP, 3), (X_UP, 0),
    (Y_DOWN, AWAY, 3), (D_SLOT, FAR, 2), (Y_DOWN, AWAY, 0), (X_LAST, 14), (R_SLOT, 10), (D_SLOT, AWAY, 1), (R_SLOT, 5),
    (Z_RELAY, 4), (Y_DOWN, AWAY, 2), (Y_DOWN, FAR, 2), (X_DOWN, 3), (Z_RELAY, 12), (Y_LAST, NEAR, 2), (Y_UP, FAR, 2),
    (Y_UP, OWN, 3), (X_DOWN, 5), (D_SLOT, FAR, 0), (X_DOWN, 4), (Y_UP, AWAY, 3), (X_UP, 1), (R_SLOT, 11), (X_UP, 15),
    (X_UP, 10), (Y_UP, NEAR, 1), (R_SLOT, 7), (X_DOWN, 6), (Y_DOWN, FAR, 0), (Y_LAST, OWN, 3), (Y_UP, AWAY, 2),
    (Y_UP, AWAY, 1), (Y_UP, FAR, 0), (Y_DOWN, NEAR, 3), (Z_RELAY, 13), (R_SLOT, 8), (Y_LAST, OWN, 1), (Y_UP, AWAY, 0),
    (Y_DOWN, FAR, 3), (X_UP, 11), (X_DOWN, 15), (X_UP, 13), (X_DOWN, 2), (Y_LAST, OWN, 2), (X_DOWN, 11), (X_UP, 5),
    (X_DOWN, 1), (Y_DOWN, AWAY, 1), (Y_LAST, AWAY, 3), (Y_LAST, OWN, 0), (X_UP, 6), (Y_LAST, NEAR, 0), (R_SLOT, 16),
    (D_SLOT, FAR, 1), (Y_LAST, NEAR, 3), (Y_UP, FAR, 1), (X_LAST, 3), (X_UP, 8), (Y_LAST, FAR, 2), (Y_UP, FAR, 3),
    (X_LAST, 15), (Y_LAST, NEAR, 1), (R_SLOT, 9), (X_DOWN, 7), (X_LAST, 13), (X_UP, 7), (X_LAST, 4), (Y_DOWN, FAR, 1),
    (X_DOWN, 8), (Y_LAST, AWAY, 0), (PREPARE, OWN), (PREPARE, NEAR), (Y_LAST, FAR, 3), (X_LAST, 0), (X_UP, 16),
    (Y_LAST, AWAY, 2), (X_DOWN, 10), (X_LAST, 2), (X_LAST, 1), (Y_LAST, FAR, 1), (Y_LAST, AWAY, 1), (MULTIPLY, OWN, 3),
    (X_LAST, 6), (X_DOWN, 16), (X_LAST, 12), (X_UP, 9), (X_DOWN, 9), (Y_LAST, FAR, 0), (MULTIPLY, OWN, 2),
    (MULTIPLY, NEAR, 2), (X_LAST, 11), (MULTIPLY, NEAR, 3), (MULTIPLY, NEAR, 1), (MULTIPLY, OWN, 0), (MULTIPLY, OWN, 1),
    (PREPARE, FAR), (X_LAST, 10), (X_LAST, 8), (X_LAST, 5), (PREPARE, AWAY), (X_LAST, 7), (X_LAST, 9), (MULTIPLY, AWAY, 1),
    (MULTIPLY, AWAY, 2), (MULTIPLY, NEAR, 0), (MULTIPLY, AWAY, 3), (MULTIPLY, FAR, 2), (MULTIPLY, AWAY, 0),
    (MULTIPLY, FAR, 3), (X_LAST, 16), (MULTIPLY, FAR, 0), (MULTIPLY, FAR, 1),
]

PIECES = (
    [(64 * s, 64) for s in range(8)]
    + [(512, 32)]
    + [(64 * s, 64) for s in range(9, 16)]
    + [(544, 32)]
)


def split(value):
    high = value.astype(BF16)
    return high, (value - high.astype(F32)).astype(BF16)


def kernel(d_hbm, r_hbm, o_ref, dv, rv, turned, dbuf, rbuf, dth, dtl, local, ss, tz, dz, dy, dd, rz, rx):
    x, zh, y, c, p = (lax.axis_index(n) for n in ("x", "zh", "y", "c", "p"))
    z = 4 * zh + p

    def ring(v, n):
        return lax.rem(v + 4 * n, n)

    def at_z(d):
        w = ring(z + d, 16)
        return {"zh": lax.div(w, 4), "p": lax.rem(w, 4)}

    up_x, down_x = {"x": ring(x + 1, 4)}, {"x": ring(x - 1, 4)}
    up_y, down_y = {"y": ring(y + 1, 4)}, {"y": ring(y - 1, 4)}
    partner = {"c": 1 - c}
    source_core = lax.div(zh, 2)
    diagonal = x == y
    holder = c == source_core
    low = p < 2

    load_d = pltpu.make_async_copy(d_hbm, dv, local.at[0])
    load_r = pltpu.make_async_copy(r_hbm, rv, local.at[1])
    own = r_hbm.at[:, pl.ds(pl.multiple_of(p * 256, 256), 256)]
    load_own = pltpu.make_async_copy(own, rbuf.at[x, pl.ds(0, 64)], local.at[2])
    load_d.start()
    load_r.start()
    load_own.start()

    barrier = pltpu.get_barrier_semaphore()

    def greet(device, when=None):
        def signal():
            pl.semaphore_signal(barrier, inc=1, device_id=device, device_id_type=MESH)

        if when is None:
            signal()
        else:
            pl.when(when)(signal)

    for d in (1, -1, 2, -2, 3, -3, 4, -4):
        greet(at_z(d))
    for device in (up_x, down_x, up_y, down_y, partner):
        greet(device)
    for other in range(4):
        greet({"x": other, "y": x}, jnp.logical_or(x != other, y != x))
    for r in (1, 3, 2):
        for ps in range(4):
            origin = {"zh": ring(zh - r, 4), "p": ps, "c": source_core}
            upward = r == 1 or (r == 2 and ps >= 2)
            greet(origin, p == (0 if upward else 3))
    o_ref[...] = jnp.zeros_like(o_ref)
    load_d.wait()
    load_own.wait()
    load_r.wait()
    pl.semaphore_wait(
        barrier,
        4 - diagonal.astype(jnp.int32) + 8 + 5 + jnp.where(holder, 2, 4),
    )

    def go(order, inner):
        started = []

        def send(src, dst, sem, device, when=None):
            copy = pltpu.make_async_remote_copy(
                src_ref=src,
                dst_ref=dst,
                send_sem=ss.at[len(started)],
                recv_sem=sem,
                device_id=device,
                device_id_type=MESH,
            )
            started.append((copy, when))
            if when is None:
                copy.start()
            else:
                pl.when(when)(copy.start)

        def arrived(dst, sem, when=None):
            copy = pltpu.make_async_copy(dst, dst, sem)
            if when is None:
                copy.wait()
            else:
                pl.when(when)(copy.wait)

        for part in range(4):
            send(
                dv.at[pl.ds(16 * part, 16)],
                turned.at[x],
                tz.at[x],
                {"x": y, "y": part},
                jnp.logical_or(x != y, y != part),
            )

        @pl.when(diagonal)
        def _():
            turned[x] = dv[pl.ds(pl.multiple_of(16 * y, 16), 16), :]

        def turned_in():
            for other in range(4):
                arrived(
                    turned.at[other],
                    tz.at[other],
                    jnp.logical_or(x != other, y != x),
                )

        def block(core, slot, part, half=None):
            first, count = (4 * slot, 4) if half is None else (4 * slot + 2 * half, 2)
            return dbuf.at[core, pl.ds(first, count), part]

        def d_send():
            for h in range(2):
                target = 2 * c + h
                rel = ring(target - zh, 4)
                up = jnp.logical_or(rel == 1, jnp.logical_and(rel == 2, p >= 2))
                entry = jnp.where(rel == 0, p, jnp.where(up, 0, 3))
                slot = 4 * rel + p
                for core in range(2):
                    columns = pl.ds(512 * h + 256 * core, 256)
                    mine = jnp.logical_and(rel == 0, c == core)
                    send(
                        turned.at[:, :, columns],
                        block(core, slot, y),
                        dz.at[slot],
                        {"zh": target, "p": entry, "c": core},
                        jnp.logical_not(mine),
                    )

                    @pl.when(mine)
                    def _():
                        dbuf[core, pl.ds(4 * p, 4), y] = turned[:, :, columns]

        ahead, behind = at_z(jnp.where(low, 1, -1)), at_z(jnp.where(low, -1, 1))
        group_of = {
            OWN: 0,
            NEAR: jnp.where(low, 1, 3),
            AWAY: jnp.where(low, 3, 1),
            FAR: 2,
        }
        here = 1 if inner else 0

        def slot_of(r, k):
            return 4 * group_of[r] + jnp.where(low, k, 3 - k)

        def d_slot(r, k):
            slot = slot_of(r, k)
            held = block(c, slot, y)
            if r == OWN and k == here:
                arrived(held, dz.at[slot], jnp.logical_not(holder))
            else:
                arrived(held, dz.at[slot])
            if r == OWN:
                goes = (k <= here, k >= here and inner)
            elif r == NEAR or (r == FAR and k >= 2):
                goes = (True, False)
            else:
                goes = (False, inner)
            for wanted, device in zip(goes, (ahead, behind)):
                if wanted:
                    send(held, held, dz.at[slot], device)
            send(held, held, dy.at[0, slot], up_y)
            send(held, held, dy.at[1, slot], down_y)
            to_partner(r, 0)

        y_of = [y, ring(y - 1, 4), ring(y + 1, 4), ring(y + 2, 4)]
        missing = {(r, which): 4 for r in group_of for which in range(4)}

        def whole(core, r, which):
            first = pl.multiple_of(16 * group_of[r], 16)
            return dbuf.at[core, pl.ds(first, 16), y_of[which]]

        def to_partner(r, which):
            missing[r, which] -= 1
            if missing[r, which] == 0:
                part = whole(c, r, which)
                send(part, part, dd.at[group_of[r], which], partner)

        def y_relay(side, r, k):
            slot, part = slot_of(r, k), y_of[1 + side]
            arrived(block(c, slot, part), dy.at[side, slot])
            half = block(c, slot, part, side)
            send(half, half, dy.at[2 + side, slot], (up_y, down_y)[side])
            to_partner(r, 1 + side)

        def y_last(r, k):
            slot = slot_of(r, k)
            for side in range(2):
                arrived(block(c, slot, y_of[3], side), dy.at[2 + side, slot])
            to_partner(r, 3)

        def piece(number, owner, half=None):
            first, count = PIECES[number]
            if half is not None:
                first, count = first + half * (count // 2), count // 2
            return rbuf.at[owner, pl.ds(first, count)]

        def z_send(d):
            quarter = pl.ds(pl.multiple_of(ring(p + d, 4) * 256, 256), 256)
            slot = (-d) % 16
            send(rv.at[:, quarter], piece(slot, x), rz.at[slot], at_z(d))

        def z_relay(number):
            side, cut = (4, 12) if number >= 12 else (-4, 4)
            half = (1 if cut == 12 else 0) if number == cut else None
            there = {12: 16, 4: 8}.get(number, number - side)
            send(piece(number, x, half), piece(there, x), rz.at[there], at_z(side))

        def along_x(number):
            for side, device in ((0, up_x), (1, down_x)):
                send(piece(number, x), piece(number, x), rx.at[side, number], device)

        def r_slot(number):
            arrived(piece(number, x), rz.at[number])
            along_x(number)

        x_of = [ring(x - 1, 4), ring(x + 1, 4), ring(x + 2, 4)]

        def x_relay(side, number):
            arrived(piece(number, x_of[side]), rx.at[side, number])
            half = piece(number, x_of[side], side)
            send(half, half, rx.at[2 + side, number], (up_x, down_x)[side])

        def x_last(number):
            for side in range(2):
                arrived(piece(number, x_of[2], side), rx.at[2 + side, number])

        def prepare(r):
            for which in range(4):
                arrived(whole(1 - c, r, which), dd.at[group_of[r], which])

            @pl.loop(0, 4)
            def _(ps):
                slot = 4 * group_of[r] + ps
                for half in range(2):
                    value = dbuf[half, pl.ds(4 * slot, 4)].reshape(256, 256).T
                    high, rest = split(value)
                    dth[slot, pl.ds(256 * half, 256), :] = high
                    dtl[slot, pl.ds(256 * half, 256), :] = rest

        def multiply(r, k):
            slot = slot_of(r, k)
            there = ring(jnp.where(low, k, 3 - k) - p - 4 * group_of[r], 16)
            rows = pl.ds(pl.multiple_of(64 * there, 64), 64)
            high, rest = split(rbuf[:, rows, :].reshape(256, 256))
            dh, dl = dth[slot], dtl[slot]
            o_ref[...] += (
                jnp.dot(dh, high, preferred_element_type=F32)
                + jnp.dot(dl, high, preferred_element_type=F32)
                + jnp.dot(dh, rest, preferred_element_type=F32)
            )

        steps = {
            X_OWN: lambda: along_x(0),
            Z_SEND: z_send,
            TURNED: turned_in,
            D_SEND: d_send,
            D_SLOT: d_slot,
            Y_UP: lambda r, k: y_relay(0, r, k),
            Y_DOWN: lambda r, k: y_relay(1, r, k),
            Y_LAST: y_last,
            R_SLOT: r_slot,
            Z_RELAY: z_relay,
            X_UP: lambda number: x_relay(0, number),
            X_DOWN: lambda number: x_relay(1, number),
            X_LAST: x_last,
            PREPARE: prepare,
            MULTIPLY: multiply,
        }
        def sent():
            for copy, when in started:
                if when is None:
                    copy.wait_send()
                else:
                    pl.when(when)(copy.wait_send)

        quiet = (X_LAST, PREPARE, MULTIPLY)
        last = max(at for at, step in enumerate(order) if step[0] not in quiet) + 1
        last = max(last, max(at for at, step in enumerate(order) if step[0] == X_LAST))
        for at, (name, *numbers) in enumerate(order):
            if at == last:
                sent()
            steps[name](*numbers)

    edge = jnp.logical_or(p == 0, p == 3)
    pl.when(edge)(lambda: go(EDGE, False))
    pl.when(jnp.logical_not(edge))(lambda: go(INNER, True))


def body(design, responses):
    dma = pltpu.SemaphoreType.DMA
    held = [pltpu.with_memory_space_constraint(v, pltpu.HBM) for v in (design, responses)]
    return pl.pallas_call(
        kernel,
        out_shape=jax.ShapeDtypeStruct((512, 256), F32),
        in_specs=[pl.BlockSpec(memory_space=pltpu.HBM)] * 2,
        out_specs=pl.BlockSpec(memory_space=pltpu.VMEM),
        scratch_shapes=[
            pltpu.VMEM((64, 1024), F32),
            pltpu.VMEM((64, 1024), F32),
            pltpu.VMEM((4, 16, 1024), F32),
            pltpu.VMEM((2, 64, 4, 16, 256), F32),
            pltpu.VMEM((4, 1024, 256), F32),
            pltpu.VMEM((16, 512, 256), BF16),
            pltpu.VMEM((16, 512, 256), BF16),
            dma((3,)),
            dma((200,)),
            dma((4,)),
            dma((16,)),
            dma((4, 16)),
            dma((4, 4)),
            dma((17,)),
            dma((4, 17)),
        ],
        compiler_params=pltpu.CompilerParams(
            collective_id=0, has_side_effects=True, vmem_limit_bytes=32 * 2**20
        ),
    )(*held)


def solution(mesh):
    finer = Mesh(
        mesh.devices.reshape(4, 4, 4, 2, 4), ("x", "zh", "y", "c", "p")
    )
    spec = P(("x", "zh", "p"), ("y", "c"))
    return jax.shard_map(
        body,
        mesh=finer,
        in_specs=(spec, spec),
        out_specs=P(("x", "zh"), ("y", "c", "p")),
        check_vma=False,
    )
```
